256 devices in a mesh: grp: 16 (over z, core), row: 16 (over y, x).
Axes of the slice: x: 4, y: 4, z: 8, core: 2. Of those that a mesh axis runs over, the one named last changes fastest.
Arguments:
- theta: float32 [32, 512, 512], P('grp', 'row'), may hold values from -8 to 8
- left_env: bfloat16 [32, 8, 512, 512], P('grp', None, 'row'), may hold values from -1.5 to 1.5
- right_env: bfloat16 [32, 8, 512, 512], P('grp', None, 'row'), may hold values from -3.5 to 3.5
- lengths: int32 [32, 2], P('grp'), may hold values from 128 to 512
Outputs:
- evolved: float32 [32, 512, 512], P('grp', 'row')
- hessenberg: float32 [8, 8], replicated
The draws below stay inside these ranges and needn't reach their ends.
All inputs are finite; a program needn't handle non-finite values.
Results may differ from the reference program's by a relative error of at most 0.0029.
Values may be sent and summed in bfloat16 or wider, within the bound.
No kernel may reach another device: no remote copies, remote signals or barrier semaphores. Data moves between devices by JAX's collectives and lax.ppermute only.
A program may use at most 64 MiB of HBM per device.

```python
import jax
import jax.numpy as jnp
from jax import lax

SECT = 512
TERMS = 8
KRYLOV = 8
SECTORS = 32


def draw_theta(key, part):
    sector_pos = jnp.arange(SECTORS, dtype=jnp.float32) / max(SECTORS - 1, 1)
    base = jnp.clip(jax.random.normal(key, (SECTORS, SECT, SECT), jnp.float32), -3.2, 3.2)
    scales = 0.4 * 6.0 ** sector_pos
    return (base * scales[:, None, None]).astype(jnp.float32)


def draw_left_env(key, part):
    noise_key = jax.random.fold_in(key, 11)
    noise = jnp.clip(jax.random.normal(noise_key, (SECTORS, TERMS, SECT, SECT), jnp.float32), -4.0, 4.0)
    noise = noise * (SECT * TERMS) ** (-0.5)
    identity = jnp.eye(SECT, dtype=jnp.float32)
    first = (jnp.arange(TERMS) == 0).astype(jnp.float32)
    return (noise + first[None, :, None, None] * identity[None, None, :, :]).astype(jnp.bfloat16)


def draw_right_env(key, part):
    noise_key = jax.random.fold_in(key, 23)
    rate_key = jax.random.fold_in(key, 37)
    noise = jnp.clip(jax.random.normal(noise_key, (SECTORS, TERMS, SECT, SECT), jnp.float32), -4.0, 4.0)
    rates = jax.random.uniform(rate_key, (SECTORS,), jnp.float32, 0.5, 2.0)
    noise = noise * SECT ** (-0.5)
    identity = jnp.eye(SECT, dtype=jnp.float32)
    first = (jnp.arange(TERMS) == 0).astype(jnp.float32)
    return (noise - (rates[:, None] * first[None, :])[:, :, None, None] * identity[None, None, :, :]).astype(jnp.bfloat16)


def plant(result, key, least, top_value):
    dims = result.shape
    place = [jax.random.randint(jax.random.fold_in(key, axis), (), 0, dims[axis]) for axis in range(len(dims))]
    result = result.at[tuple(place)].set(least)
    longest = dims.index(max(dims))
    place[longest] = (place[longest] + 1) % dims[longest]
    return result.at[tuple(place)].set(top_value)


def setup_inputs(seed: int = 0) -> dict:
    key_list = jax.random.split(jax.random.key(seed), 5)
    return {
        "theta": draw_theta(jax.random.fold_in(key_list[4], 71), 0),
        "left_env": draw_left_env(jax.random.fold_in(key_list[4], 71), 0),
        "right_env": draw_right_env(jax.random.fold_in(key_list[4], 71), 0),
        "lengths": plant(jax.random.randint(key_list[3], (SECTORS, 2), SECT // 4, SECT + 1), jax.random.fold_in(key_list[3], 1), SECT // 4, SECT).astype(jnp.int32),
    }


epsilon = 1e-06
time_step = 0.5

def live_of(lengths):
    row_ids = lax.broadcasted_iota(jnp.int32, (1, SECT, 1), 1)
    col_ids = lax.broadcasted_iota(jnp.int32, (1, 1, SECT), 2)
    return ((row_ids < lengths[:, 0][:, None, None]) & (col_ids < lengths[:, 1][:, None, None])).astype(jnp.float32)

def apply_sector(operands):
    vector, left_one, right_one = operands
    packed = lax.optimization_barrier(vector.astype(jnp.bfloat16)).astype(jnp.float32)
    inner_terms = jnp.einsum('ab,wbc->wac', packed, right_one.astype(jnp.float32), precision=lax.Precision.HIGHEST)
    inner_terms = lax.optimization_barrier(inner_terms.astype(jnp.bfloat16)).astype(jnp.float32)
    return jnp.einsum('wba,wbc->ac', left_one.astype(jnp.float32), inner_terms, precision=lax.Precision.HIGHEST)

def propagate(hessenberg):
    scaled = time_step * hessenberg
    series = jnp.eye(KRYLOV, dtype=jnp.float32)
    series_term = jnp.eye(KRYLOV, dtype=jnp.float32)
    for degree in range(1, 19):
        series_term = jnp.dot(series_term, scaled, precision=lax.Precision.HIGHEST) / degree
        series = series + series_term
    return series[:, 0]

def reference(theta, left_env, right_env, lengths):
    live_mask = live_of(lengths)
    start_block = theta * live_mask
    norm_zero = jnp.sqrt(jnp.sum(start_block * start_block) + epsilon)
    krylov_basis = [start_block / norm_zero]
    hessenberg = jnp.zeros((KRYLOV, KRYLOV), jnp.float32)
    for column in range(KRYLOV):
        image = lax.map(apply_sector, (krylov_basis[column], left_env, right_env)) * live_mask
        coefficients = jnp.stack([jnp.sum(vector * image) for vector in krylov_basis])
        for previous in range(column + 1):
            image = image - coefficients[previous] * krylov_basis[previous]
        hessenberg = hessenberg.at[:column + 1, column].set(coefficients)
        if column + 1 < KRYLOV:
            beta_norm = jnp.sqrt(jnp.sum(image * image) + epsilon)
            hessenberg = hessenberg.at[column + 1, column].set(beta_norm)
            krylov_basis.append(image / beta_norm)
    weights = propagate(hessenberg)
    evolved = jnp.zeros_like(start_block)
    for column in range(KRYLOV):
        evolved = evolved + weights[column] * krylov_basis[column]
    return (norm_zero * evolved, hessenberg)
```

```python
import functools

import jax
import jax.numpy as jnp
from jax import lax
from jax.experimental import pallas as pl
from jax.experimental.pallas import tpu as pltpu
from jax.sharding import Mesh
from jax.sharding import PartitionSpec as P


KRYLOV = 8
NZ, NC, NY, NX = 8, 2, 4, 4
ROW = ("row_0", "row_1")
GRP = ("grp_0", "grp_1")
OWNERS = ("grp_0", "grp_1", "row_1")
BLK = 64
HS = 16
CANCEL = 0.01

epsilon = 1e-06
time_step = 0.5
BF = jnp.bfloat16
F32 = jnp.float32


def safe_inverse(value):
    return jnp.where(value > 0, 1.0 / jnp.where(value > 0, value, 1.0), 0.0)


def chain_kernel(ints, norm_ref, *refs):
    one, many = refs[:5], refs[5:10]
    hs_ref, q_out = refs[10], refs[11:15]
    rv, lv, lt, inner, basis, image, packed, hi, lo, sems, out_sems = refs[15:]
    terms, size = rv.shape[:2]
    owner, yid, xid, len_row, len_col = (ints[i] for i in range(5))
    norm0 = norm_ref[0]

    def rows_of(dy, k):
        return pl.multiple_of(32 * (4 * lax.rem(yid + dy, 4) + lax.rem(xid + 4 - k, 4)), 32)

    hs_ref[...] = jnp.zeros(hs_ref.shape, F32)

    @pl.when(owner == 1)
    def _():
        copies_r, copies_l = [], []

        def add(src, dst, into):
            copy = pltpu.make_async_copy(src, dst, sems.at[len(copies_r) + len(copies_l)])
            copy.start()
            into.append(copy)

        for k in range(4):
            for dy, ref, r_at, l_at in zip((0, 3, 1, 2, 2), one if k == 0 else many, (0, 0, 0, 0, None), (9, 9, 9, None, 0)):
                ref = ref if k == 0 else ref.at[k - 1]
                rows = pl.ds(rows_of(dy, k), 32)
                if l_at is not None:
                    add(ref.at[pl.ds(l_at + 1, terms)], lv.at[:, rows, :], copies_l)
                    add(ref.at[l_at], lo.at[rows], copies_r)
                if r_at is not None:
                    add(ref.at[pl.ds(r_at + 1, terms)], rv.at[:, rows, :], copies_r)
                    add(ref.at[r_at], hi.at[rows], copies_r)
        for copy in copies_l:
            copy.wait()
        row_ids = lax.broadcasted_iota(jnp.int32, (size, size), 0)
        col_ids = lax.broadcasted_iota(jnp.int32, (size, size), 1)
        eye = jnp.where(row_ids == col_ids, 1.0, 0.0).astype(BF)
        for w in range(terms):
            turned = lax.dot_general(eye, lv[w], (((1,), (1,)), ((), ())), preferred_element_type=F32)
            lt[:, w * size : (w + 1) * size] = turned.astype(BF)
        for copy in copies_r:
            copy.wait()

        def blocks(fn, init):
            return lax.fori_loop(0, size // BLK, lambda b, c: fn(pl.ds(pl.multiple_of(b * BLK, BLK), BLK), b, c), init)

        def live(b):
            r = b * BLK + lax.broadcasted_iota(jnp.int32, (BLK, size), 0)
            c = lax.broadcasted_iota(jnp.int32, (BLK, size), 1)
            return (r < len_row) & (c < len_col)

        def lanes(t, op):
            return op(op(t[:, 0:128], t[:, 128:256]), op(t[:, 256:384], t[:, 384:512]))

        def fold(x):
            return lanes(jnp.sum(x.reshape(BLK // 8, 8, size), axis=0), jnp.add)

        zero = jnp.zeros((8, 128), F32)
        none = jnp.zeros((1, 1), F32)

        def load_start(rows, b, top):
            x = jnp.where(live(b), hi[rows].astype(F32) + lo[rows].astype(F32), 0.0)
            image[rows] = x
            packed[rows] = (x / norm0).astype(BF)
            return jnp.maximum(top, lanes(jnp.max(jnp.abs(x).reshape(BLK // 8, 8, size), axis=0), jnp.maximum))

        top = jnp.max(blocks(load_start, zero), keepdims=True)
        top_inv = safe_inverse(top)

        def square(rows, b, acc):
            x = image[rows] * top_inv
            return acc + fold(x * x)

        start_len = jnp.sqrt(jnp.sum(blocks(square, zero), keepdims=True))
        start_inv = safe_inverse(start_len)
        nu = top * start_len / norm0
        nu_inv = safe_inverse(nu)

        def first(rows, b, c):
            basis[0, rows] = image[rows] * top_inv * start_inv
            return c

        blocks(first, 0)
        lane = lax.broadcasted_iota(jnp.int32, (8, 128), 1)
        hs_ref[...] = jnp.where(lane == HS - 1, nu, 0.0)

        def send_rows(k):
            rows = pl.ds(pl.multiple_of(128 * yid + 32 * lax.rem(xid + k, 4), 32), 32)
            return pltpu.make_async_copy(basis.at[:, rows, :], q_out[k], out_sems.at[k])

        def orthogonalise(j):
            last = j + 1 == KRYLOV

            def dots(rows, b, accs, fresh=True, squares=True):
                u = image[rows]
                if fresh:
                    u = jnp.where(live(b), u, 0.0)
                    if j == 0:
                        u = u * nu_inv
                    image[rows] = u
                news = [acc + fold(u * basis[i, rows]) for i, acc in enumerate(accs[: j + 1])]
                return tuple(news + ([accs[-1] + fold(u * u)] if squares else []))

            sums = blocks(functools.partial(dots, squares=not last), (zero,) * (j + 1 + (not last)))
            coef = [jnp.sum(s, keepdims=True) for s in sums]
            if not last:
                whole = coef.pop()
                left = whole
                for c in coef:
                    left = left - c * c

                def take(rows, b, acc, coef):
                    u = image[rows]
                    for i in range(j + 1):
                        u = u - coef[i] * basis[i, rows]
                    image[rows] = u
                    return acc + fold(u * u)

                def twice():
                    blocks(functools.partial(take, coef=coef), zero)
                    more = blocks(functools.partial(dots, fresh=False, squares=False), (zero,) * (j + 1))
                    more = [jnp.sum(s, keepdims=True) for s in more]
                    rest = jnp.sum(blocks(functools.partial(take, coef=more), zero), keepdims=True)
                    return (rest, *[none] * (j + 1), *[c + e for c, e in zip(coef, more)])

                again = jnp.sum(jnp.where(left < CANCEL * whole, 1.0, 0.0)) > 0.5
                left, *both = lax.cond(again, twice, lambda: (left, *coef, *coef))
                off, coef = both[: j + 1], both[j + 1 :]
                beta = jnp.sqrt(left)
                beta_inv = safe_inverse(beta)
                hs_ref[...] += jnp.where(lane == HS * j + j + 1, beta, 0.0)

                def step(rows, b, c):
                    u = image[rows]
                    for i in range(j + 1):
                        u = u - off[i] * basis[i, rows]
                    u = u * beta_inv
                    basis[j + 1, rows] = u
                    packed[rows] = u.astype(BF)
                    return c

                blocks(step, 0)
                if j + 2 == KRYLOV:
                    for k in range(4):
                        send_rows(k).start()
            for i in range(j + 1):
                hs_ref[...] += jnp.where(lane == HS * j + i, coef[i], 0.0)

        def column(j, carry):
            for w in range(terms):
                q = jnp.dot(packed[...], rv[w], preferred_element_type=F32)
                inner[w * size : (w + 1) * size, :] = q.astype(BF)
            for m in range(2):
                rows = slice(m * size // 2, (m + 1) * size // 2)
                image[rows] = jnp.dot(lt[rows, :], inner[...], preferred_element_type=F32)
            for known in range(KRYLOV):
                pl.when(j == known)(functools.partial(orthogonalise, known))
            return carry

        lax.fori_loop(0, KRYLOV, column, 0)
        for k in range(4):
            send_rows(k).wait()


def chain(ints, norm0, shards, terms, size):
    hbm = pl.BlockSpec(memory_space=pltpu.HBM)
    smem = pl.BlockSpec(memory_space=pltpu.SMEM)
    return pl.pallas_call(
        chain_kernel,
        out_shape=(jax.ShapeDtypeStruct((8, 128), F32),) + (jax.ShapeDtypeStruct((KRYLOV, 32, size), F32),) * 4,
        in_specs=[smem, smem] + [hbm] * 10,
        out_specs=(pl.BlockSpec(memory_space=pltpu.VMEM),) + (hbm,) * 4,
        scratch_shapes=[
            pltpu.VMEM((terms, size, size), BF),
            pltpu.VMEM((terms, size, size), BF),
            pltpu.VMEM((size, terms * size), BF),
            pltpu.VMEM((terms * size, size), BF),
            pltpu.VMEM((KRYLOV, size, size), F32),
            pltpu.VMEM((size, size), F32),
            pltpu.VMEM((size, size), BF),
            pltpu.VMEM((size, size), BF),
            pltpu.VMEM((size, size), BF),
            pltpu.SemaphoreType.DMA((64,)),
            pltpu.SemaphoreType.DMA((4,)),
        ],
        compiler_params=pltpu.CompilerParams(vmem_limit_bytes=48 * 1024 * 1024),
        name="chain",
    )(ints, norm0, *shards)


def finish_kernel(ints, norm_ref, got, *refs):
    arrived, evolved, hess_ref = refs[:4], *refs[4:]
    members = got.shape[0]
    xid, core, first = ints[2], ints[5], ints[6]
    norm0 = norm_ref[0]
    table = jnp.concatenate([got[:, 0, :], jnp.zeros((128 - members, 128), F32)], axis=0).T
    rows = lax.broadcasted_iota(jnp.int32, (HS, 128), 0)
    lanes = lax.broadcasted_iota(jnp.int32, (HS, 128), 1)
    steps = []
    nu = jnp.sum(jnp.where(rows == HS - 1, table[0:HS], 0.0), axis=0, keepdims=True)
    for k in range(KRYLOV):
        steps.append(jnp.where(rows < HS - 1, table[HS * k : HS * k + HS], 0.0))
    basis = [jnp.where(rows == 0, nu, 0.0)]
    r8 = lax.broadcasted_iota(jnp.int32, (8, 128), 0)
    c8 = lax.broadcasted_iota(jnp.int32, (8, 128), 1)
    hess = jnp.zeros((8, 128), F32)
    turned = jnp.zeros((8, 128), F32)

    def total(x):
        return jnp.sum(jnp.sum(x, axis=0, keepdims=True), axis=1, keepdims=True)

    for j in range(KRYLOV):
        u = jnp.zeros((HS, 128), F32)
        for k in range(j + 1):
            u = u + steps[k] * basis[j][k : k + 1, :]
        coef = [total(b * u) for b in basis]
        for i in range(j + 1):
            u = u - coef[i] * basis[i]
            hess = hess + jnp.where((r8 == i) & (c8 == j), coef[i], 0.0)
            turned = turned + jnp.where((r8 == j) & (c8 == i), coef[i], 0.0)
        if j + 1 < KRYLOV:
            beta = jnp.sqrt(total(u * u) + epsilon)
            hess = hess + jnp.where((r8 == j + 1) & (c8 == j), beta, 0.0)
            turned = turned + jnp.where((r8 == j) & (c8 == j + 1), beta, 0.0)
            basis.append(u / beta)
    hess_ref[...] = hess[:, :KRYLOV]
    scaled = time_step * hess
    scaled_turned = time_step * turned
    as_row = jnp.where((lax.broadcasted_iota(jnp.int32, (1, 128), 1) == 0), 1.0, 0.0)
    weights = jnp.where(lax.broadcasted_iota(jnp.int32, (8, 1), 0) == 0, 1.0, 0.0)
    weights_row = jnp.zeros((1, 128), F32)
    for degree in range(1, 19):
        if degree % 2:
            as_col = jnp.sum(scaled * as_row, axis=1, keepdims=True) / degree
            weights = weights + as_col
        else:
            as_row = jnp.sum(scaled_turned * as_col, axis=0, keepdims=True) / degree
            weights_row = weights_row + as_row
    weights = weights + jnp.sum(jnp.where(r8 == c8, weights_row, 0.0), axis=1, keepdims=True)
    coords = jnp.zeros((HS, 128), F32)
    for j in range(KRYLOV):
        coords = coords + weights[j : j + 1, :] * basis[j]
    for k, ref in enumerate(arrived):
        source = lax.rem(xid + 4 - k, 4)
        place = source - 2 * core

        @pl.when((place >= 0) & (place < 2))
        def _():
            mine = norm0 * jnp.sum(jnp.where(lanes == first + source, coords, 0.0), axis=1, keepdims=True)
            acc = mine[0:1, :] * ref[0]
            for i in range(1, KRYLOV):
                acc = acc + mine[i : i + 1, :] * ref[i]
            evolved[place] = acc


def finish(ints, norm0, got, arrived):
    smem = pl.BlockSpec(memory_space=pltpu.SMEM)
    vmem = pl.BlockSpec(memory_space=pltpu.VMEM)
    return pl.pallas_call(
        finish_kernel,
        out_shape=(
            jax.ShapeDtypeStruct((2, *arrived[0].shape[1:]), F32),
            jax.ShapeDtypeStruct((KRYLOV, KRYLOV), F32),
        ),
        in_specs=[smem, smem] + [vmem] * 5,
        out_specs=(vmem, vmem),
        name="finish",
    )(ints, norm0, got, *arrived)


def summed(value, axes, members):
    sent = jnp.broadcast_to(value, (members, 8, 128))
    return jnp.sum(lax.all_to_all(sent, axes, 0, 0, tiled=True)[:, 0, 0])


def local(theta, left_env, right_env, lengths):
    zid, core, yid, xid = (lax.axis_index(a) for a in ("grp_0", "grp_1", "row_0", "row_1"))
    local_rows, size = theta.shape[1:]
    terms = left_env.shape[1]
    high = lax.reduce_precision(theta, 8, 7)
    low = (theta - high).astype(BF)
    high = high.astype(BF)
    whole = jnp.concatenate([high[:, None], right_env, low[:, None], left_env], axis=1)
    half = terms + 1

    def for_shift(k):
        place = jnp.clip((xid + k) % NX - 2 * core, 0, 1)
        return lax.dynamic_index_in_dim(whole, place, 0, keepdims=False)

    def across(value, k):
        pairs = [(c * NX + (x - k) % NX, c * NX + x) for c in range(NC) for x in (2 * c, 2 * c + 1)]
        return lax.ppermute(value, ("grp_1", "row_1"), pairs)

    def around(value, shift):
        def at(c, y, x):
            return (c * NY + y % NY) * NX + x

        pairs = [(at(c, y, x), at(c, y + shift, x)) for c in range(NC) for y in range(NY) for x in (2 * c, 2 * c + 1)]
        return lax.ppermute(value, ("grp_1", "row_0", "row_1"), pairs)

    others = [across(for_shift(k), k) for k in (1, 3, 2)]
    own = for_shift(0)
    below, above = around(own, 1), around(own, -1)
    one = [own, below, above, around(below[:half], 1), around(above[half:], -1)]
    row_ids = (yid * NX + xid) * local_rows + lax.broadcasted_iota(jnp.int32, (1, local_rows, 1), 1)
    col_ids = lax.broadcasted_iota(jnp.int32, (1, 1, size), 2)
    live = (row_ids < lengths[:, 0][:, None, None]) & (col_ids < lengths[:, 1][:, None, None])
    start = jnp.where(live, theta, 0.0)
    column_sq = summed(jnp.sum(start * start), GRP, NZ * NC)
    tie = jnp.minimum(column_sq, 0.0).astype(BF)
    bundle = jnp.stack([others[0], others[2], others[1]]) + tie
    below, above = around(bundle, 1), around(bundle, -1)
    whole_sq = summed(column_sq, ROW, NY * NX)
    norm0 = jnp.sqrt(whole_sq + epsilon)
    tie = jnp.minimum(whole_sq, 0.0).astype(BF)
    many = [bundle, below, above, around(below[:, :half] + tie, 1), around(above[:, half:] + tie, -1)]

    owner = (xid // 2 == core).astype(jnp.int32)
    live_len = lax.dynamic_index_in_dim(lengths, jnp.clip(xid - 2 * core, 0, 1), 0, keepdims=False)
    ints = jnp.stack([owner, yid, xid, live_len[0], live_len[1], core, (zid * NC + core) * NX]).astype(jnp.int32)
    norm_vec = norm0.reshape(1)
    found, *rows = chain(ints, norm_vec, one + many, terms, size)
    arrived = [rows[0]]
    for k in range(1, NX):
        pairs = [(c * NX + x, c * NX + (x + k) % NX) for c in range(NC) for x in (2 * c, 2 * c + 1)]
        arrived.append(lax.ppermute(rows[k], ("grp_1", "row_1"), pairs))
    members = NZ * NC * NX
    got = lax.all_to_all(jnp.broadcast_to(found[None], (members, 8, 128)), OWNERS, 0, 0, tiled=True)
    return finish(ints, norm_vec, got, arrived)


def solution(mesh):
    finer = Mesh(mesh.devices.reshape(NZ, NC, NY, NX), ("grp_0", "grp_1", "row_0", "row_1"))
    return jax.shard_map(
        local,
        mesh=finer,
        in_specs=(
            P(GRP, ROW, None),
            P(GRP, None, ROW, None),
            P(GRP, None, ROW, None),
            P(GRP, None),
        ),
        out_specs=(P(GRP, ROW, None), P()),
        check_vma=False,
    )
```

```python
import functools

import jax
import jax.numpy as jnp
from jax import lax
from jax.experimental import pallas as pl
from jax.experimental.pallas import tpu as pltpu
from jax.sharding import Mesh
from jax.sharding import PartitionSpec as P


KRYLOV = 8
NZ, NC, NY, NX = 8, 2, 4, 4
ROW = ("row_0", "row_1")
GRP = ("grp_0", "grp_1")
OWNERS = ("grp_0", "grp_1", "row_1")
BLK = 64
HS = 16
CANCEL = 0.01

epsilon = 1e-06
time_step = 0.5
BF = jnp.bfloat16
F32 = jnp.float32


def safe_inverse(value):
    return jnp.where(value > 0, 1.0 / jnp.where(value > 0, value, 1.0), 0.0)


def chain_kernel(ints, *refs):
    pieces, far, far2 = refs[:9], refs[9:11], refs[11:13]
    hs_ref, q_out = refs[13], refs[14:18]
    rv, lv, lt, inner, basis, image, packed, packed_low, hi, lo, sems, out_sems = refs[18:]
    terms, size = rv.shape[:2]
    owner, yid, xid, len_row, len_col = (ints[i] for i in range(5))

    def rows_of(dy, k):
        return pl.multiple_of(32 * (4 * lax.rem(yid + dy, 4) + lax.rem(xid + 4 - k, 4)), 32)

    hs_ref[...] = jnp.zeros(hs_ref.shape, F32)

    @pl.when(owner == 1)
    def _():
        copies_r, copies_l = [], []

        def add(src, dst, into):
            copy = pltpu.make_async_copy(src, dst, sems.at[len(copies_r) + len(copies_l)])
            copy.start()
            into.append(copy)

        places = []
        for k, (at, n) in enumerate(((0, None), (1, 0), (2, None), (1, 1))):
            own, below, above = (ref if n is None else ref.at[:, n] for ref in (pieces[3 * at + i] for i in range(3)))
            far_r, far_l = far2 if k == 2 else [ref.at[(0, 1, None, 2)[k]] for ref in far]
            for dy, from_r, from_l in (
                (0, own.at[0], own.at[1]),
                (3, below.at[0], below.at[1]),
                (1, above.at[0], above.at[1]),
                (2, far_r, far_l),
            ):
                places.append((pl.ds(rows_of(dy, k), 32), from_r, from_l))
        for rows, _, from_l in places:
            add(from_l.at[pl.ds(1, terms)], lv.at[:, rows, :], copies_l)
        for rows, from_r, from_l in places:
            add(from_r.at[0], hi.at[rows], copies_r)
            add(from_l.at[0], lo.at[rows], copies_r)
            add(from_r.at[pl.ds(1, terms)], rv.at[:, rows, :], copies_r)
        for copy in copies_l:
            copy.wait()
        row_ids = lax.broadcasted_iota(jnp.int32, (size, size), 0)
        col_ids = lax.broadcasted_iota(jnp.int32, (size, size), 1)
        eye = jnp.where((row_ids == col_ids) & (row_ids < len_row), 1.0, 0.0).astype(BF)
        alive = jnp.where(lax.broadcasted_iota(jnp.int32, (1, size), 1) < len_col, 1.0, 0.0)
        for w in range(terms):
            turned = lax.dot_general(eye, lv[w], (((1,), (1,)), ((), ())), preferred_element_type=F32)
            lt[:, w * size : (w + 1) * size] = turned.astype(BF)
        for copy in copies_r:
            copy.wait()

        def blocks(fn, init):
            return lax.fori_loop(0, size // BLK, lambda b, c: fn(pl.ds(pl.multiple_of(b * BLK, BLK), BLK), b, c), init)

        def live(b):
            r = b * BLK + lax.broadcasted_iota(jnp.int32, (BLK, size), 0)
            c = lax.broadcasted_iota(jnp.int32, (BLK, size), 1)
            return (r < len_row) & (c < len_col)

        def lanes(t, op):
            return op(op(t[:, 0:128], t[:, 128:256]), op(t[:, 256:384], t[:, 384:512]))

        def fold(x):
            return lanes(jnp.sum(x.reshape(BLK // 8, 8, size), axis=0), jnp.add)

        zero = jnp.zeros((8, 128), F32)
        none = jnp.zeros((1, 1), F32)

        def load_start(rows, b, top):
            keep = live(b)
            high = jnp.where(keep, hi[rows].astype(F32), 0.0)
            low = jnp.where(keep, lo[rows].astype(F32), 0.0)
            x = high + low
            image[rows] = x
            packed[rows] = high.astype(BF)
            packed_low[rows] = low.astype(BF)
            return jnp.maximum(top, lanes(jnp.max(jnp.abs(x).reshape(BLK // 8, 8, size), axis=0), jnp.maximum))

        top = jnp.max(blocks(load_start, zero), keepdims=True)
        top_inv = safe_inverse(top)

        def square(rows, b, acc):
            x = image[rows] * top_inv
            return acc + fold(x * x)

        start_len = jnp.sqrt(jnp.sum(blocks(square, zero), keepdims=True))
        start_inv = safe_inverse(start_len)
        nu = top * start_len
        nu_inv = safe_inverse(nu)

        def first(rows, b, c):
            basis[0, rows] = image[rows] * top_inv * start_inv
            return c

        blocks(first, 0)
        lane = lax.broadcasted_iota(jnp.int32, (8, 128), 1)
        hs_ref[...] = jnp.where(lane == HS - 1, nu, 0.0)

        def send_rows(k):
            rows = pl.ds(pl.multiple_of(128 * yid + 32 * lax.rem(xid + k, 4), 32), 32)
            return pltpu.make_async_copy(basis.at[:, rows, :], q_out[k], out_sems.at[k])

        def orthogonalise(j):
            last = j + 1 == KRYLOV
            before = alive * nu_inv if j == 0 else alive

            def dots(rows, b, accs, fresh=True, squares=True):
                u = image[rows]
                if fresh:
                    u = u * before
                news = [acc + fold(u * basis[i, rows]) for i, acc in enumerate(accs[: j + 1])]
                return tuple(news + ([accs[-1] + fold(u * u)] if squares else []))

            sums = blocks(functools.partial(dots, squares=not last), (zero,) * (j + 1 + (not last)))
            coef = [jnp.sum(s, keepdims=True) for s in sums]
            if not last:
                whole = coef.pop()
                left = whole
                for c in coef:
                    left = left - c * c

                def take(rows, b, acc, coef, fresh=True):
                    u = image[rows]
                    if fresh:
                        u = u * before
                    for i in range(j + 1):
                        u = u - coef[i] * basis[i, rows]
                    image[rows] = u
                    return acc + fold(u * u)

                def twice():
                    blocks(functools.partial(take, coef=coef), zero)
                    more = blocks(functools.partial(dots, fresh=False, squares=False), (zero,) * (j + 1))
                    more = [jnp.sum(s, keepdims=True) for s in more]
                    rest = jnp.sum(blocks(functools.partial(take, coef=more, fresh=False), zero), keepdims=True)
                    return (rest, jnp.ones((1, size), F32), *[none] * (j + 1), *[c + e for c, e in zip(coef, more)])

                again = jnp.sum(jnp.where(left < CANCEL * whole, 1.0, 0.0)) > 0.5
                left, before, *both = lax.cond(again, twice, lambda: (left, before, *coef, *coef))
                off, coef = both[: j + 1], both[j + 1 :]
                beta = jnp.sqrt(left)
                beta_inv = safe_inverse(beta)
                hs_ref[...] += jnp.where(lane == HS * j + j + 1, beta, 0.0)

                def step(rows, b, c):
                    u = image[rows] * before
                    for i in range(j + 1):
                        u = u - off[i] * basis[i, rows]
                    u = u * beta_inv
                    basis[j + 1, rows] = u
                    packed[rows] = u.astype(BF)
                    return c

                blocks(step, 0)
                if j + 2 == KRYLOV:
                    for k in range(NX):
                        send_rows(k).start()
            for i in range(j + 1):
                hs_ref[...] += jnp.where(lane == HS * j + i, coef[i], 0.0)

        def stage_one(low):
            for w in range(terms):
                q = jnp.dot(packed[...], rv[w], preferred_element_type=F32)
                if low:
                    q = q + jnp.dot(packed_low[...], rv[w], preferred_element_type=F32)
                inner[w * size : (w + 1) * size, :] = q.astype(BF)

        def column(j, carry):
            pl.when(j == 0)(functools.partial(stage_one, True))
            pl.when(j > 0)(functools.partial(stage_one, False))
            for m in range(2):
                rows = slice(m * size // 2, (m + 1) * size // 2)
                image[rows] = jnp.dot(lt[rows, :], inner[...], preferred_element_type=F32)
            for known in range(KRYLOV):
                pl.when(j == known)(functools.partial(orthogonalise, known))
            return carry

        lax.fori_loop(0, KRYLOV, column, 0)
        for k in range(NX):
            send_rows(k).wait()


def chain(ints, shards, terms, size):
    hbm = pl.BlockSpec(memory_space=pltpu.HBM)
    smem = pl.BlockSpec(memory_space=pltpu.SMEM)
    return pl.pallas_call(
        chain_kernel,
        out_shape=(jax.ShapeDtypeStruct((8, 128), F32),) + (jax.ShapeDtypeStruct((KRYLOV, 32, size), F32),) * NX,
        in_specs=[smem] + [hbm] * 13,
        out_specs=(pl.BlockSpec(memory_space=pltpu.VMEM),) + (hbm,) * NX,
        scratch_shapes=[
            pltpu.VMEM((terms, size, size), BF),
            pltpu.VMEM((terms, size, size), BF),
            pltpu.VMEM((size, terms * size), BF),
            pltpu.VMEM((terms * size, size), BF),
            pltpu.VMEM((KRYLOV, size, size), F32),
            pltpu.VMEM((size, size), F32),
            pltpu.VMEM((size, size), BF),
            pltpu.VMEM((size, size), BF),
            pltpu.VMEM((size, size), BF),
            pltpu.VMEM((size, size), BF),
            pltpu.SemaphoreType.DMA((64,)),
            pltpu.SemaphoreType.DMA((NX,)),
        ],
        compiler_params=pltpu.CompilerParams(vmem_limit_bytes=48 * 1024 * 1024),
        name="chain",
    )(ints, *shards)


def finish_kernel(ints, got, *refs):
    arrived, evolved, hess_ref = refs[:NX], *refs[NX:]
    members = got.shape[0]
    xid, core, first = ints[2], ints[5], ints[6]
    table = jnp.concatenate([got[:, 0, :], jnp.zeros((128 - members, 128), F32)], axis=0).T
    rows = lax.broadcasted_iota(jnp.int32, (HS, 128), 0)
    lanes = lax.broadcasted_iota(jnp.int32, (HS, 128), 1)
    steps = []
    nu = jnp.sum(jnp.where(rows == HS - 1, table[0:HS], 0.0), axis=0, keepdims=True)
    for k in range(KRYLOV):
        steps.append(jnp.where(rows < HS - 1, table[HS * k : HS * k + HS], 0.0))

    def total(x):
        return jnp.sum(jnp.sum(x, axis=0, keepdims=True), axis=1, keepdims=True)

    norm0 = jnp.sqrt(total(nu * nu) + epsilon)
    basis = [jnp.where(rows == 0, nu / norm0, 0.0)]
    r8 = lax.broadcasted_iota(jnp.int32, (8, 128), 0)
    c8 = lax.broadcasted_iota(jnp.int32, (8, 128), 1)
    hess = jnp.zeros((8, 128), F32)
    turned = jnp.zeros((8, 128), F32)

    for j in range(KRYLOV):
        u = jnp.zeros((HS, 128), F32)
        for k in range(j + 1):
            u = u + steps[k] * basis[j][k : k + 1, :]
        coef = [total(b * u) for b in basis]
        for i in range(j + 1):
            u = u - coef[i] * basis[i]
            hess = hess + jnp.where((r8 == i) & (c8 == j), coef[i], 0.0)
            turned = turned + jnp.where((r8 == j) & (c8 == i), coef[i], 0.0)
        if j + 1 < KRYLOV:
            beta = jnp.sqrt(total(u * u) + epsilon)
            hess = hess + jnp.where((r8 == j + 1) & (c8 == j), beta, 0.0)
            turned = turned + jnp.where((r8 == j) & (c8 == j + 1), beta, 0.0)
            basis.append(u / beta)
    hess_ref[...] = hess[:, :KRYLOV]
    scaled = time_step * hess
    scaled_turned = time_step * turned
    as_row = jnp.where((lax.broadcasted_iota(jnp.int32, (1, 128), 1) == 0), 1.0, 0.0)
    weights = jnp.where(lax.broadcasted_iota(jnp.int32, (8, 1), 0) == 0, 1.0, 0.0)
    weights_row = jnp.zeros((1, 128), F32)
    for degree in range(1, 19):
        if degree % 2:
            as_col = jnp.sum(scaled * as_row, axis=1, keepdims=True) / degree
            weights = weights + as_col
        else:
            as_row = jnp.sum(scaled_turned * as_col, axis=0, keepdims=True) / degree
            weights_row = weights_row + as_row
    weights = weights + jnp.sum(jnp.where(r8 == c8, weights_row, 0.0), axis=1, keepdims=True)
    coords = jnp.zeros((HS, 128), F32)
    for j in range(KRYLOV):
        coords = coords + weights[j : j + 1, :] * basis[j]
    for k, ref in enumerate(arrived):
        source = lax.rem(xid + 4 - k, 4)
        place = source - 2 * core

        @pl.when((place >= 0) & (place < 2))
        def _():
            mine = norm0 * jnp.sum(jnp.where(lanes == first + source, coords, 0.0), axis=1, keepdims=True)
            acc = mine[0:1, :] * ref[0]
            for i in range(1, KRYLOV):
                acc = acc + mine[i : i + 1, :] * ref[i]
            evolved[place] = acc


def finish(ints, got, arrived):
    smem = pl.BlockSpec(memory_space=pltpu.SMEM)
    vmem = pl.BlockSpec(memory_space=pltpu.VMEM)
    return pl.pallas_call(
        finish_kernel,
        out_shape=(
            jax.ShapeDtypeStruct((2, *arrived[0].shape[1:]), F32),
            jax.ShapeDtypeStruct((KRYLOV, KRYLOV), F32),
        ),
        in_specs=[smem] + [vmem] * 5,
        out_specs=(vmem, vmem),
        name="finish",
    )(ints, got, *arrived)


def local(theta, left_env, right_env, lengths):
    zid, core, yid, xid = (lax.axis_index(a) for a in ("grp_0", "grp_1", "row_0", "row_1"))
    _, size = theta.shape[1:]
    terms = left_env.shape[1]
    high = lax.reduce_precision(theta, 8, 7)
    low = (theta - high).astype(BF)
    high = high.astype(BF)
    right = jnp.concatenate([high[:, None], right_env], axis=1)
    left = jnp.concatenate([low[:, None], left_env], axis=1)
    whole = jnp.stack([right, left], axis=1)

    def for_shift(k):
        place = jnp.clip((xid + k) % NX - 2 * core, 0, 1)
        return lax.dynamic_index_in_dim(whole, place, 0, keepdims=False)

    def across(value, k):
        pairs = [(c * NX + (x - k) % NX, c * NX + x) for c in range(NC) for x in (2 * c, 2 * c + 1)]
        return lax.ppermute(value, ("grp_1", "row_1"), pairs)

    def around(value, shift):
        def at(c, y, x):
            return (c * NY + y % NY) * NX + x

        pairs = [(at(c, y, x), at(c, y + shift, x)) for c in range(NC) for y in range(NY) for x in (2 * c, 2 * c + 1)]
        return lax.ppermute(value, ("grp_1", "row_0", "row_1"), pairs)

    second = across(for_shift(2), 2)
    first = across(for_shift(1), 1)
    third = across(for_shift(3), 3)
    own = for_shift(0)
    below = around(own, 1)
    above = around(own, -1)
    first, third, below, above = lax.optimization_barrier((first, third, below, above))
    sides = jnp.stack([first, third], axis=1)
    below1 = around(sides, 1)
    above1 = around(sides, -1)
    below2 = around(second, 1)
    above2 = around(second, -1)
    pieces = [own, below, above, sides, below1, above1, second, below2, above2]
    far = [
        around(jnp.concatenate([below[0][None], below1[0]]), 1),
        around(jnp.concatenate([above[1][None], above1[1]]), -1),
    ]
    far2 = [around(below2[0], 1), around(above2[1], -1)]

    owner = (xid // 2 == core).astype(jnp.int32)
    live_len = lax.dynamic_index_in_dim(lengths, jnp.clip(xid - 2 * core, 0, 1), 0, keepdims=False)
    ints = jnp.stack([owner, yid, xid, live_len[0], live_len[1], core, (zid * NC + core) * NX]).astype(jnp.int32)
    found, *rows = chain(ints, pieces + far + far2, terms, size)
    arrived = [rows[0]]
    members = NZ * NC * NX
    got = lax.all_to_all(jnp.broadcast_to(found[None], (members, 8, 128)), OWNERS, 0, 0, tiled=True)
    for k in range(1, NX):
        pairs = [(c * NX + x, c * NX + (x + k) % NX) for c in range(NC) for x in (2 * c, 2 * c + 1)]
        arrived.append(lax.ppermute(rows[k], ("grp_1", "row_1"), pairs))
    return finish(ints, got, arrived)


def solution(mesh):
    finer = Mesh(mesh.devices.reshape(NZ, NC, NY, NX), ("grp_0", "grp_1", "row_0", "row_1"))
    return jax.shard_map(
        local,
        mesh=finer,
        in_specs=(
            P(GRP, ROW, None),
            P(GRP, None, ROW, None),
            P(GRP, None, ROW, None),
            P(GRP, None),
        ),
        out_specs=(P(GRP, ROW, None), P()),
        check_vma=False,
    )
```
